32 devices in a mesh: parts: 2 (over y), blk: 4 (over x, core), sub: 4 (over z).
Axes of the slice: x: 2, y: 2, z: 4, core: 2. Of those that a mesh axis runs over, the one named last changes fastest.
Arguments:
- tokens: bfloat16 [256, 4096], P(('parts', 'blk'), 'sub'), parts along dimension 0, may hold values from -6 to 6
- expert_ids: int32 [256, 2], P(('parts', 'blk')), parts along dimension 0, may hold values from 0 to 7, all different within a row; in each aligned block of 32 rows (0 to 31, 32 to 63, ...) at most 16 rows name the same one
- gate_level: int32 [256, 2], P(('parts', 'blk')), parts along dimension 0, may hold values from 0 to 15
- gate_weight: bfloat16 [8, 4096, 8192], P('blk', None, 'sub'), may hold values from -0.09375 to 0.09375
- up_weight: bfloat16 [8, 4096, 8192], P('blk', None, 'sub'), may hold values from -0.09375 to 0.09375
- down_weight: bfloat16 [8, 8192, 4096], P('blk', 'sub'), may hold values from -0.0625 to 0.0625
Outputs:
- mixed_out: bfloat16 [256, 4096], P(('parts', 'blk'), 'sub'), parts along dimension 0
The draws below stay inside these ranges and needn't reach their ends.
There are 2 independent parts, one for each index of `parts`. The reference program is written for one: setup_inputs(seed, part) draws one part's arguments, and reference() takes and returns one part's arrays. A program takes and returns all parts, laid end to end along the dimension named above; an argument that names none is the same for every part. Nothing has to cross between parts.
Inputs may be any that keep to these rules, and one draw needn't show every extreme that they name: `expert_ids`: A token's 2 experts differ. Among the 32 tokens of one index of blk (aligned blocks of tokens), no expert is picked by more than 16 tokens, and in some block some expert is picked by exactly 16.
All inputs are finite; a program needn't handle non-finite values.
Results may differ from the reference program's by a relative error of at most 0.015.
Values may be sent and summed in bfloat16 or wider, within the bound.
A program may use at most 192 MiB of HBM per device.

```python
import math
import jax
import jax.numpy as jnp
import numpy as np
from jax import lax

D = 4096
E = 8
TOP = 2
FF = 8192
LEVELS = 16
TOK_BLK = 32
FSPLIT = 1
SLOTS = 8
SLOT_FF = 8192
CAP = 16
TOKENS = 128
N_BLK = 4


def with_ends(array, rng, smallest, high):
    longest = array.shape.index(max(array.shape))
    spots = []
    for shift in (0, 1):
        where = [jax.random.randint(jax.random.fold_in(rng, axis), (), 0, length) for axis, length in enumerate(array.shape)]
        where[longest] = (where[longest] + shift) % array.shape[longest]
        spots.append(tuple(where))
    return array.at[spots[0]].set(smallest).at[spots[1]].set(high)


def steps_of(stream_key, shape, split, smallest, high):
    def one(dim, parts):
        draws = jax.random.uniform(jax.random.fold_in(jax.random.fold_in(stream_key, 6), dim), (parts,), jnp.float32, smallest / len(split), high / len(split))
        return jnp.repeat(jnp.exp(draws), shape[dim] // parts).reshape((-1,) + (1,) * (len(shape) - dim - 1))

    level = one(*split[0])
    for cut in split[1:]:
        level = level * one(*cut)
    return level


def routed_block(key, own, number, rows, amount, top, bound, slope):
    order = jax.random.permutation(key, amount)
    crowded, ordinary = load_shares(amount, rows * top, bound, slope, True), load_shares(amount, rows * top, bound, slope, False)
    places = jnp.arange(amount)

    def named(sizes, rotation):
        used = int((sizes > 0).sum())
        fixed = max(1, used // 4)
        passed = fixed + (places - fixed + rotation * (used - fixed)) % max(1, amount - fixed)
        return jnp.zeros((amount,), jnp.int32).at[order[jnp.where(places < fixed, places, passed)]].set(jnp.asarray(sizes, jnp.int32))

    sizes = jnp.where(number % 4 == 0, named(crowded, number // 4), named(ordinary, number - number // 4 - 1))
    mixed = jax.random.permutation(jax.random.fold_in(own, 3), amount)
    source_of, sink = mixed[0:amount // 2 * 2:2], mixed[1:amount // 2 * 2:2]
    room = jnp.minimum(sizes[source_of] - 1, bound - sizes[sink]) // 2
    room = jnp.where((source_of == order[0]) | (sink == order[0]) | (sizes[sink] == 0), 0, jnp.maximum(room, 0))
    passed = jax.random.randint(jax.random.fold_in(own, 4), (amount // 2,), 0, 1 << 20) % (room + 1)
    sizes = sizes.at[source_of].add(-passed).at[sink].add(passed)
    labels = jnp.searchsorted(jnp.cumsum(sizes), jnp.arange(rows * top), side="right").astype(jnp.int32)
    listing = labels.reshape(top, rows).T
    listing = listing[jax.random.permutation(jax.random.fold_in(own, 1), rows)]
    rotation = jax.random.randint(jax.random.fold_in(own, 2), (rows, 1), 0, top)
    return jnp.take_along_axis(listing, (jnp.arange(top)[None, :] + rotation) % top, axis=1)


def load_shares(count, total, bound, slope, full):
    weights = [(1 << 20) // math.isqrt(rank ** slope) + 1 for rank in range(1, count + 1)]
    largest = bound if full else min(bound, max(-(-total // count), total * weights[0] // sum(weights)))
    least = 1 if total - largest >= count - 1 else 0
    holding, surplus = [largest] + [least] * (count - 1), total - largest - least * (count - 1)
    while surplus > 0:
        free = [i for i in range(1, count) if holding[i] < largest] or [i for i in range(1, count) if holding[i] < bound]
        pool, budget = sum([weights[i] for i in free]), surplus
        for i in free:
            extra = min(bound - holding[i], max(1, budget * weights[i] // pool), surplus)
            holding[i] = holding[i] + extra
            surplus = surplus - extra
    return np.array(holding)


def centred(key, extent, spread, most, shards=(), kind=jnp.bfloat16):
    entries = jax.random.normal(key, extent, jnp.float32) * spread
    if len(shards) > 0:
        entries = steps_of(key, extent, shards, -0.22, 0.18) * entries
    return jnp.clip(entries, min=-most, max=most).astype(kind)


def setup_inputs(seed: int = 0, part: int = 0) -> dict:
    streams_of = jax.random.split(jax.random.key(seed), 7)
    part_splits = jax.random.split(jax.random.fold_in(streams_of[6], part), 7)
    tokens = centred(part_splits[0], (TOKENS, D), 1.0, 6.0, ((0, 4), (1, 4)))
    expert_ids_keys = jax.random.split(jax.random.fold_in(part_splits[1], 1), TOKENS // TOK_BLK)
    expert_ids_turns = jax.random.permutation(jax.random.fold_in(part_splits[1], 3), TOKENS // TOK_BLK)
    expert_ids = jax.vmap(lambda own, number: routed_block(jax.random.fold_in(part_splits[1], 2), own, number, TOK_BLK, E, TOP, CAP, 2))(expert_ids_keys, expert_ids_turns).reshape((TOKENS, TOP))
    gate_level = with_ends(jax.random.randint(part_splits[2], (TOKENS, TOP), 0, LEVELS), jax.random.fold_in(part_splits[2], 1), 0, LEVELS - 1).astype(jnp.int32)
    gate_weight = centred(streams_of[3], (SLOTS, D, SLOT_FF), D ** -0.5, 0.09375, ((0, 4), (2, 4)))
    up_weight = centred(streams_of[4], (SLOTS, D, SLOT_FF), D ** -0.5, 0.09375, ((0, 4), (2, 4)))
    down_weight = centred(streams_of[5], (SLOTS, SLOT_FF, D), FF ** -0.5, 0.0625, ((0, 4), (1, 4)))
    return {"tokens": tokens, "expert_ids": expert_ids, "gate_level": gate_level, "gate_weight": gate_weight, "up_weight": up_weight, "down_weight": down_weight}


def reference(tokens, expert_ids, gate_level, gate_weight, up_weight, down_weight):
    picked = expert_ids.reshape(N_BLK, TOK_BLK * TOP)
    onehot = (picked[:, :, None] == jnp.arange(E, dtype=jnp.int32)[None, None, :]).astype(jnp.int32)
    ranking = jnp.sum((jnp.cumsum(onehot, axis=1) - onehot) * onehot, axis=2)
    block_index = jnp.arange(N_BLK, dtype=jnp.int32)[:, None]
    position = (block_index * CAP + ranking).reshape(-1).astype(jnp.int32)
    flat_expert = expert_ids.reshape(-1).astype(jnp.int32)
    token_index = jnp.repeat(jnp.arange(TOKENS, dtype=jnp.int32), TOP)
    row_table = jnp.full((E, N_BLK * CAP), TOKENS, jnp.int32).at[flat_expert, position].set(token_index)
    padded = jnp.concatenate([tokens, jnp.zeros((1, D), tokens.dtype)], axis=0)

    def one_slot(slot_index):
        expert = slot_index % E
        slot_rows = padded[row_table[expert]]
        gate_acts = jnp.dot(slot_rows, gate_weight[slot_index], preferred_element_type=jnp.float32)
        up_acts = jnp.dot(slot_rows, up_weight[slot_index], preferred_element_type=jnp.float32)
        hidden = (jax.nn.silu(gate_acts) * up_acts).astype(jnp.bfloat16)
        return jnp.dot(hidden, down_weight[slot_index], preferred_element_type=jnp.float32).astype(jnp.bfloat16)

    slot_out = lax.map(one_slot, jnp.arange(SLOTS, dtype=jnp.int32))
    expert_sum = jnp.sum(slot_out.astype(jnp.float32).reshape(FSPLIT, E, N_BLK * CAP, D), axis=0)
    levels = gate_level.astype(jnp.float32) + 1.0
    shares = levels / jnp.sum(levels, axis=1, keepdims=True)
    gathered = expert_sum[flat_expert, position].reshape(TOKENS, TOP, D)
    mixed_out = jnp.sum(gathered * shares[:, :, None], axis=1)
    return mixed_out.astype(jnp.bfloat16)
```

```python
import contextlib
import functools

import jax
import jax.numpy as jnp
from jax import lax
from jax.sharding import PartitionSpec as P

from jax.experimental import pallas as pl
from jax.experimental.pallas import tpu as pltpu

E = 8
TOP = 2
CAP = 16
BF16 = jnp.bfloat16
F32 = jnp.float32
TILE = 1024
AHEAD = 3
SCOPES = False


def scope(name):
    return jax.named_scope(name) if SCOPES else contextlib.nullcontext()


def shards(tokens, expert_ids, gate_level, gate_weight, up_weight, down_weight):
    block_count = lax.axis_size("blk")
    sub_count = lax.axis_size("sub")
    local_slots = gate_weight.shape[0]
    hidden_width = gate_weight.shape[2]
    slot_count = local_slots * block_count
    halves = slot_count // E
    token_rows = tokens.shape[0]
    feature_width = tokens.shape[1]
    buffer_width = slot_count * CAP
    received_rows = block_count * CAP
    picked = expert_ids.reshape(-1)
    onehot = (picked[:, None] == jnp.arange(E, dtype=jnp.int32)[None, :]).astype(jnp.int32)
    ranking = jnp.sum((jnp.cumsum(onehot, axis=0) - onehot) * onehot, axis=1)
    columns = (
        picked[:, None] * CAP
        + (jnp.arange(halves, dtype=jnp.int32) * E)[None, :] * CAP
        + ranking[:, None]
    )
    columns = columns.reshape(token_rows, TOP * halves)
    matches = columns[:, :, None] == jnp.arange(buffer_width, dtype=jnp.int32)[None, None, :]
    levels = gate_level.astype(jnp.float32) + 1.0
    shares = levels / jnp.sum(levels, axis=1, keepdims=True)
    shares_wide = jnp.repeat(shares, halves, axis=1)
    combine_weights = jnp.sum(matches.astype(jnp.float32) * shares_wide[:, :, None], axis=1)
    chosen = jnp.any(matches, axis=1).astype(jnp.bfloat16)
    outgoing = lax.dot_general(
        chosen, tokens, (((0,), (0,)), ((), ())), preferred_element_type=jnp.float32
    )
    outgoing = outgoing.astype(jnp.bfloat16).reshape(slot_count, CAP, feature_width)
    copies = jnp.broadcast_to(
        outgoing.reshape(block_count, 1, local_slots, CAP, feature_width),
        (block_count, sub_count, local_slots, CAP, feature_width),
    )
    copies = copies.reshape(block_count * sub_count, local_slots, CAP, feature_width)
    arrived = lax.all_to_all(copies, ("blk", "sub"), split_axis=0, concat_axis=0, tiled=True)
    arrived = arrived.reshape(block_count, sub_count, local_slots, CAP, feature_width)
    gate_split = gate_weight.reshape(local_slots, sub_count, feature_width, hidden_width)
    up_split = up_weight.reshape(local_slots, sub_count, feature_width, hidden_width)
    gate_acts = jnp.einsum(
        "bsncd,nsdf->nbcf", arrived, gate_split, preferred_element_type=jnp.float32
    )
    up_acts = jnp.einsum("bsncd,nsdf->nbcf", arrived, up_split, preferred_element_type=jnp.float32)
    gate_acts = gate_acts.reshape(local_slots, received_rows, hidden_width)
    up_acts = up_acts.reshape(local_slots, received_rows, hidden_width)
    hidden = (jax.nn.silu(gate_acts) * up_acts).astype(jnp.bfloat16)
    full_out = jnp.einsum("nrf,nfd->nrd", hidden, down_weight, preferred_element_type=jnp.float32)
    local_out = lax.psum_scatter(
        full_out.astype(jnp.bfloat16), "sub", scatter_dimension=2, tiled=True
    )
    home_rows = lax.all_to_all(local_out, "blk", split_axis=1, concat_axis=0, tiled=True)
    home_flat = home_rows.reshape(buffer_width, feature_width).astype(jnp.float32)
    mixed_out = jnp.dot(
        combine_weights,
        home_flat,
        precision=lax.Precision.HIGHEST,
        preferred_element_type=jnp.float32,
    )
    return mixed_out.astype(jnp.bfloat16)


def flip(index, mask, count):
    total, bit = 0, 1
    while bit < count:
        digit = (index // bit) % 2
        total = total + bit * ((1 - digit) if mask & bit else digit)
        bit *= 2
    return total


def fused(
    parts, blks, subs, tokens_hbm, ids_hbm, levels_hbm, gate_hbm, up_hbm, down_hbm, out,
    ids, levels, taken, picked, rows, both, down_rest, down_edge, gate_sum, up_sum, hidden, made, home, mixed, landed, edge_sum, edges,
    load_sem, down_sem, own_sem, tok_send, tok_recv, pick_send, pick_recv, made_send, made_recv, mix_send, mix_recv, relay_send, relay_recv, edge_send, edge_recv,
):
    plane = parts * blks
    part, blk, sub = lax.axis_index("parts"), lax.axis_index("blk"), lax.axis_index("sub")
    mine = blk * parts + part
    block_rows, width = tokens_hbm.shape
    units = hidden.shape[1]

    def at(slot, depth):
        return {"parts": slot % parts, "blk": slot // parts, "sub": depth}

    near = width // 4
    far = pl.ds(near, width - near)
    quarters = [flip(sub, j, subs) for j in range(subs)]
    peers = [flip(mine, k, plane) for k in range(plane)]

    def send(source, target, send_sem, recv_sem, to):
        return pltpu.make_async_remote_copy(
            src_ref=source, dst_ref=target, send_sem=send_sem, recv_sem=recv_sem,
            device_id=to, device_id_type=pl.DeviceIdType.MESH,
        )

    def arrived(ref, sem):
        send(ref, ref, sem, sem, at(mine, sub)).wait_recv()

    def departed(ref, sem):
        send(ref, ref, sem, sem, at(mine, sub)).wait_send()

    others = pl.ds(0, plane - 1)
    barrier = pltpu.get_barrier_semaphore()
    for k in range(1, plane):
        pl.semaphore_signal(barrier, inc=1, device_id=at(peers[k], sub), device_id_type=pl.DeviceIdType.MESH)
    for j in range(1, subs):
        pl.semaphore_signal(barrier, inc=1, device_id=at(mine, quarters[j]), device_id_type=pl.DeviceIdType.MESH)
    small = [
        pltpu.make_async_copy(source, target, own_sem.at[n])
        for n, (source, target) in enumerate([(ids_hbm, ids), (levels_hbm, levels), (tokens_hbm, taken.at[0])])
    ]
    for copy in small:
        copy.start()

    slim = width // 4
    edge, rest = pl.ds(0, slim), pl.ds(slim, width - slim)
    loads = []
    for j in range(subs):
        span = pl.ds(pl.multiple_of(quarters[j] * width, width), width)
        loads.append([
            pltpu.make_async_copy(source.at[part, span, :], both.at[i, j], load_sem.at[j])
            for i, source in enumerate((gate_hbm, up_hbm))
        ])
    for j in reversed(range(subs)):
        span = pl.ds(pl.multiple_of(quarters[j] * width + slim, slim), width - slim)
        loads.append([pltpu.make_async_copy(down_hbm.at[part, :, span], down_rest.at[j], down_sem.at[j])])
        if j == subs - 1:
            loads.append([
                pltpu.make_async_copy(
                    down_hbm.at[part, :, pl.ds(pl.multiple_of(quarters[i] * width, width), slim)],
                    down_edge.at[:, pl.ds(i * slim, slim)],
                    down_sem.at[subs],
                )
                for i in range(subs)
            ])

    def load(count):
        for group in loads[:count]:
            for copy in group:
                copy.start()
        del loads[:count]

    for copy in small:
        copy.wait()
    load(AHEAD)

    lines = E * CAP
    line = lax.broadcasted_iota(jnp.int32, (lines, block_rows), 0)
    expert, place = line // CAP, line % CAP
    first = jnp.broadcast_to(ids[0:1, :], (lines, block_rows)) == expert
    second = jnp.broadcast_to(ids[1:2, :], (lines, block_rows)) == expert
    named = jnp.where(first | second, 1.0, 0.0).astype(F32)
    before = lax.broadcasted_iota(jnp.int32, (block_rows, block_rows), 0) < lax.broadcasted_iota(
        jnp.int32, (block_rows, block_rows), 1
    )
    rank = jnp.dot(named.astype(BF16), jnp.where(before, 1.0, 0.0).astype(BF16), preferred_element_type=F32)
    here = jnp.where(rank == place.astype(F32), named, 0.0)
    chosen = here.astype(BF16)

    with scope("barrier"):
        pl.semaphore_wait(barrier, plane + subs - 2)

    tok_copies = {}
    for j in range(1, subs):
        tok_copies[j] = send(
            taken.at[0, :, far], taken.at[j, :, far], tok_send, tok_recv.at[j - 1], at(mine, quarters[j])
        )
        tok_copies[j].start()

    half = width // 2
    spans_in = [(0, 0, near), (0, near, width - near)]
    spans_in += [(j, near, width - near) for j in range(1, subs - 1)]
    spans_in += [(subs - 1, near, half - near), (subs - 1, half, half)]

    def dispatch(n, j, start, size):
        span = pl.ds(start, size)
        if j > 0 and start == near:
            tok_copies[j].wait_recv()
        sent = jnp.dot(chosen, taken[j, :, span], preferred_element_type=F32)
        picked[j, :, :, span] = sent.astype(BF16).reshape(plane, CAP, size)
        for k in reversed(range(1, plane)):
            send(
                picked.at[j, peers[k], :, span], rows.at[j, mine, :, span], pick_send.at[min(n, 1)], pick_recv.at[n], at(peers[k], sub)
            ).start()
        rows[j, mine, :, span] = picked[j, mine, :, span]

    def gathered(n):
        j, start, size = spans_in[n]
        arrived(rows.at[j, others, :, pl.ds(start, size)], pick_recv.at[n])

    for n, piece in enumerate(spans_in[:2]):
        dispatch(n, *piece)
    with scope("pick0"):
        gathered(0)
    relays = {}
    for j in range(1, subs):
        relays[j] = send(
            rows.at[0, :, :, pl.ds(0, near)], rows.at[j, :, :, pl.ds(0, near)],
            relay_send, relay_recv.at[j - 1], at(mine, quarters[j]),
        )
        relays[j].start()
    level = levels[...].astype(F32) + 1.0
    share = level / (level[0:1, :] + level[1:2, :])
    weight = here * jnp.where(
        first,
        jnp.broadcast_to(share[0:1, :], (lines, block_rows)),
        jnp.broadcast_to(share[1:2, :], (lines, block_rows)),
    )
    weight = weight.T
    weight_high = weight.astype(BF16)
    weight_low = (weight - weight_high.astype(F32)).astype(BF16)

    spans_used = [(j, 0, width) for j in range(subs - 1)] + [(subs - 1, 0, half), (subs - 1, half, half)]

    def absorb(n):
        j, start, size = spans_used[n]
        if start == 0:
            if j > 0:
                with scope(f"relay{j}"):
                    relays[j].wait_recv()
            with scope(f"load{j}"):
                arrived(both.at[:, j], load_sem.at[j])
            load(1)
        with scope(f"pick{n + 1}"):
            gathered(n + 1)
        depth = pl.ds(start, size)

        def tile(span):
            x = rows[j, :, :, depth].reshape(plane * CAP, size)
            g = jnp.dot(x, both[0, j, depth, span], preferred_element_type=F32)
            u = jnp.dot(x, both[1, j, depth, span], preferred_element_type=F32)
            if n > 0:
                g = g + gate_sum[:, span]
                u = u + up_sum[:, span]
            if n < len(spans_used) - 1:
                gate_sum[:, span] = g
                up_sum[:, span] = u
            else:
                hidden[:, span] = (g / (1.0 + jnp.exp(-g)) * u).astype(BF16)

        with scope(f"absorb{n}"):
            for step in range(units // TILE):
                tile(pl.ds(step * TILE, TILE))

    for n, piece in enumerate(spans_in[2:]):
        if n == subs - 2:
            absorb(0)
        dispatch(n + 2, *piece)
    for n in range(1, len(spans_used)):
        absorb(n)
    load(len(loads))

    edge_copies = {}
    mix_copies = {}

    def ship(n, j, span):
        for k in reversed(range(1, plane)):
            send(
                made.at[j, peers[k], :, span], home.at[j, mine, :, span], made_send.at[n // subs], made_recv.at[n], at(peers[k], sub)
            ).start()
        home[j, mine, :, span] = made[j, mine, :, span]

    def combine(n, j, span):
        with scope(f"madewait{n}"):
            arrived(home.at[j, others, :, span], made_recv.at[n])
        block = home[j, :, :, span].reshape(plane * CAP, span.size)
        return jnp.dot(weight_high, block, preferred_element_type=F32) + jnp.dot(
            weight_low, block, preferred_element_type=F32
        )

    for j in reversed(range(subs)):
        with scope(f"down{j}"):
            arrived(down_rest.at[j], down_sem.at[j])
            product = jnp.dot(hidden[...], down_rest[j], preferred_element_type=F32)
            made[j, :, :, rest] = product.astype(BF16).reshape(plane, CAP, width - slim)
            ship(j, j, rest)
        if j < subs - 1:
            continue
        with scope("edge"):
            arrived(down_edge, down_sem.at[subs])
            product = jnp.dot(hidden[...], down_edge[...], preferred_element_type=F32)
            edge_sum[...] = product[:, :slim]
            for i in reversed(range(1, subs)):
                made[i, :, :, edge] = product[:, i * slim : (i + 1) * slim].astype(BF16).reshape(plane, CAP, slim)
                edge_copies[i] = send(
                    made.at[i, :, :, edge], edges.at[i], edge_send, edge_recv.at[i - 1], at(mine, quarters[i])
                )
                edge_copies[i].start()

    def mix(j):
        mixed[j] = combine(j, j, rest).astype(BF16)
        mix_copies[j] = send(mixed.at[j], landed.at[j], mix_send, mix_recv.at[j - 1], at(mine, quarters[j]))
        mix_copies[j].start()

    for j in reversed(range(2, subs)):
        mix(j)
    sums = edge_sum[...]
    with scope("edgewait"):
        for j in range(1, subs):
            edge_copies[j].wait_recv()
            sums = sums + edges[j].reshape(plane * CAP, slim).astype(F32)
    made[0, :, :, edge] = sums.astype(BF16).reshape(plane, CAP, slim)
    ship(subs, 0, edge)
    mix(1)
    total = combine(0, 0, rest)
    for j in reversed(range(1, subs)):
        with scope(f"mixwait{j}"):
            mix_copies[j].wait_recv()
        total = total + landed[j].astype(F32)
    out[:, rest] = total.astype(BF16)
    out[:, edge] = combine(subs, 0, edge).astype(BF16)

    with scope("sends"):
        remote = pl.ds(1, subs - 1)
        departed(taken.at[remote, :, far], tok_send)
        departed(rows.at[remote, :, :, pl.ds(0, near)], relay_send)
        departed(edges.at[remote], edge_send)
        departed(landed.at[remote], mix_send)
        departed(rows.at[0, others, :, pl.ds(0, near)], pick_send.at[0])
        departed(rows.at[:, others, :, far], pick_send.at[1])
        departed(home.at[:, others, :, rest], made_send.at[0])
        departed(home.at[0, others, :, edge], made_send.at[1])


def shared_shards(parts, blks, subs, tokens, expert_ids, gate_level, gate_weight, up_weight, down_weight):
    block_rows, width = tokens.shape
    plane = parts * blks
    units = gate_weight.shape[2]
    vmem = pl.BlockSpec(memory_space=pltpu.VMEM)
    hbm = pl.BlockSpec(memory_space=pl.ANY)
    dma = pltpu.SemaphoreType.DMA
    return pl.pallas_call(
        functools.partial(fused, parts, blks, subs),
        out_shape=pltpu.VMEM((block_rows, width), BF16),
        in_specs=[hbm] * 6,
        out_specs=vmem,
        scratch_shapes=[
            pltpu.VMEM(expert_ids.T.shape, jnp.int32),
            pltpu.VMEM(gate_level.T.shape, jnp.int32),
            pltpu.VMEM((subs, block_rows, width), BF16),
            pltpu.VMEM((subs, plane, CAP, width), BF16),
            pltpu.VMEM((subs, plane, CAP, width), BF16),
            pltpu.VMEM((2, subs, width, units), BF16),
            pltpu.VMEM((subs, units, width - width // 4), BF16),
            pltpu.VMEM((units, subs * (width // 4)), BF16),
            pltpu.VMEM((plane * CAP, units), F32),
            pltpu.VMEM((plane * CAP, units), F32),
            pltpu.VMEM((plane * CAP, units), BF16),
            pltpu.VMEM((subs, plane, CAP, width), BF16),
            pltpu.VMEM((subs, plane, CAP, width), BF16),
            pltpu.VMEM((subs, block_rows, width - width // 4), BF16),
            pltpu.VMEM((subs, block_rows, width - width // 4), BF16),
            pltpu.VMEM((plane * CAP, width // 4), F32),
            pltpu.VMEM((subs, plane, CAP, width // 4), BF16),
            dma((subs,)), dma((subs + 1,)), dma((3,)),
            dma, dma((subs - 1,)),
            dma((2,)), dma((subs + 2,)),
            dma((2,)), dma((subs + 1,)),
            dma, dma((subs - 1,)),
            dma, dma((subs - 1,)),
            dma, dma((subs - 1,)),
        ],
        compiler_params=pltpu.CompilerParams(
            collective_id=0, has_side_effects=True, vmem_limit_bytes=65000000
        ),
    )(tokens, expert_ids.T, gate_level.T, gate_weight, up_weight, down_weight)


def routed(parts, blks, subs, tokens, expert_ids, gate_level, gate_weight, up_weight, down_weight):
    plane = parts * blks
    width = tokens.shape[1]
    units = gate_weight.shape[2]
    fits = gate_weight.shape[0] == parts and plane == E and plane & (plane - 1) == 0
    fits = fits and subs & (subs - 1) == 0 and width % TILE == 0 and units % TILE == 0
    fits = fits and tokens.shape[0] == 2 * CAP
    arrays = (tokens, expert_ids, gate_level, gate_weight, up_weight, down_weight)
    return shared_shards(parts, blks, subs, *arrays) if fits else shards(*arrays)


def solution(mesh):
    sizes = (mesh.shape["parts"], mesh.shape["blk"], mesh.shape["sub"])
    return jax.shard_map(
        functools.partial(routed, *sizes),
        mesh=mesh,
        in_specs=(
            P(("parts", "blk"), "sub"),
            P(("parts", "blk"), None),
            P(("parts", "blk"), None),
            P("blk", None, "sub"),
            P("blk", None, "sub"),
            P("blk", "sub", None),
        ),
        out_specs=P(("parts", "blk"), "sub"),
        check_vma=False,
    )
```

```python
import contextlib
import functools

import jax
import jax.numpy as jnp
from jax import lax
from jax.sharding import PartitionSpec as P

from jax.experimental import pallas as pl
from jax.experimental.pallas import tpu as pltpu

E = 8
TOP = 2
CAP = 16
BF16 = jnp.bfloat16
F32 = jnp.float32
TILE = 1024
AHEAD = 3
NEAR = 2
SLIM = 2
SCOPES = False


def scope(name):
    return jax.named_scope(name) if SCOPES else contextlib.nullcontext()


def shards(tokens, expert_ids, gate_level, gate_weight, up_weight, down_weight):
    block_count = lax.axis_size("blk")
    sub_count = lax.axis_size("sub")
    local_slots = gate_weight.shape[0]
    hidden_width = gate_weight.shape[2]
    slot_count = local_slots * block_count
    halves = slot_count // E
    token_rows = tokens.shape[0]
    feature_width = tokens.shape[1]
    buffer_width = slot_count * CAP
    received_rows = block_count * CAP
    picked = expert_ids.reshape(-1)
    onehot = (picked[:, None] == jnp.arange(E, dtype=jnp.int32)[None, :]).astype(jnp.int32)
    ranking = jnp.sum((jnp.cumsum(onehot, axis=0) - onehot) * onehot, axis=1)
    columns = (
        picked[:, None] * CAP
        + (jnp.arange(halves, dtype=jnp.int32) * E)[None, :] * CAP
        + ranking[:, None]
    )
    columns = columns.reshape(token_rows, TOP * halves)
    matches = columns[:, :, None] == jnp.arange(buffer_width, dtype=jnp.int32)[None, None, :]
    levels = gate_level.astype(jnp.float32) + 1.0
    shares = levels / jnp.sum(levels, axis=1, keepdims=True)
    shares_wide = jnp.repeat(shares, halves, axis=1)
    combine_weights = jnp.sum(matches.astype(jnp.float32) * shares_wide[:, :, None], axis=1)
    chosen = jnp.any(matches, axis=1).astype(jnp.bfloat16)
    outgoing = lax.dot_general(
        chosen, tokens, (((0,), (0,)), ((), ())), preferred_element_type=jnp.float32
    )
    outgoing = outgoing.astype(jnp.bfloat16).reshape(slot_count, CAP, feature_width)
    copies = jnp.broadcast_to(
        outgoing.reshape(block_count, 1, local_slots, CAP, feature_width),
        (block_count, sub_count, local_slots, CAP, feature_width),
    )
    copies = copies.reshape(block_count * sub_count, local_slots, CAP, feature_width)
    arrived = lax.all_to_all(copies, ("blk", "sub"), split_axis=0, concat_axis=0, tiled=True)
    arrived = arrived.reshape(block_count, sub_count, local_slots, CAP, feature_width)
    gate_split = gate_weight.reshape(local_slots, sub_count, feature_width, hidden_width)
    up_split = up_weight.reshape(local_slots, sub_count, feature_width, hidden_width)
    gate_acts = jnp.einsum(
        "bsncd,nsdf->nbcf", arrived, gate_split, preferred_element_type=jnp.float32
    )
    up_acts = jnp.einsum("bsncd,nsdf->nbcf", arrived, up_split, preferred_element_type=jnp.float32)
    gate_acts = gate_acts.reshape(local_slots, received_rows, hidden_width)
    up_acts = up_acts.reshape(local_slots, received_rows, hidden_width)
    hidden = (jax.nn.silu(gate_acts) * up_acts).astype(jnp.bfloat16)
    full_out = jnp.einsum("nrf,nfd->nrd", hidden, down_weight, preferred_element_type=jnp.float32)
    local_out = lax.psum_scatter(
        full_out.astype(jnp.bfloat16), "sub", scatter_dimension=2, tiled=True
    )
    home_rows = lax.all_to_all(local_out, "blk", split_axis=1, concat_axis=0, tiled=True)
    home_flat = home_rows.reshape(buffer_width, feature_width).astype(jnp.float32)
    mixed_out = jnp.dot(
        combine_weights,
        home_flat,
        precision=lax.Precision.HIGHEST,
        preferred_element_type=jnp.float32,
    )
    return mixed_out.astype(jnp.bfloat16)


def flip(index, mask, count):
    total, bit = 0, 1
    while bit < count:
        digit = (index // bit) % 2
        total = total + bit * ((1 - digit) if mask & bit else digit)
        bit *= 2
    return total


def fused(
    parts, blks, subs, tokens_hbm, ids_hbm, levels_hbm, gate_hbm, up_hbm, down_hbm, out,
    ids, levels, taken, picked, rows, both, down_rest, down_edge, gate_sum, up_sum, hidden, made, home, mixed, landed, edge_sum, edges, placed,
    load_sem, down_sem, own_sem, tok_send, tok_recv, pick_send, pick_recv, made_send, made_recv, mix_send, mix_recv, relay_send, relay_recv, edge_send, edge_recv,
):
    plane = parts * blks
    part, blk, sub = lax.axis_index("parts"), lax.axis_index("blk"), lax.axis_index("sub")
    mine = blk * parts + part
    block_rows, width = tokens_hbm.shape
    units = hidden.shape[1]

    def at(slot, depth):
        return {"parts": slot % parts, "blk": slot // parts, "sub": depth}

    near = width * NEAR // 8
    far = pl.ds(near, width - near)
    quarters = [flip(sub, j, subs) for j in range(subs)]
    peers = [flip(mine, k, plane) for k in range(plane)]

    def send(source, target, send_sem, recv_sem, to):
        return pltpu.make_async_remote_copy(
            src_ref=source, dst_ref=target, send_sem=send_sem, recv_sem=recv_sem,
            device_id=to, device_id_type=pl.DeviceIdType.MESH,
        )

    def arrived(ref, sem):
        send(ref, ref, sem, sem, at(mine, sub)).wait_recv()

    def departed(ref, sem):
        send(ref, ref, sem, sem, at(mine, sub)).wait_send()

    others = pl.ds(0, plane - 1)
    barrier = pltpu.get_barrier_semaphore()
    for k in range(1, plane):
        pl.semaphore_signal(barrier, inc=1, device_id=at(peers[k], sub), device_id_type=pl.DeviceIdType.MESH)
    for j in range(1, subs):
        pl.semaphore_signal(barrier, inc=1, device_id=at(mine, quarters[j]), device_id_type=pl.DeviceIdType.MESH)
    small = [
        pltpu.make_async_copy(source, target, own_sem.at[n])
        for n, (source, target) in enumerate([(ids_hbm, ids), (levels_hbm, levels), (tokens_hbm, taken.at[0])])
    ]
    for copy in small:
        copy.start()

    slim = width * SLIM // 8
    edge, rest = pl.ds(0, slim), pl.ds(slim, width - slim)
    loads = []
    for j in range(subs):
        span = pl.ds(pl.multiple_of(quarters[j] * width, width), width)
        loads.append([
            pltpu.make_async_copy(source.at[part, span, :], both.at[i, j], load_sem.at[j])
            for i, source in enumerate((gate_hbm, up_hbm))
        ])
    loads.append([
        pltpu.make_async_copy(
            down_hbm.at[part, :, pl.ds(pl.multiple_of(quarters[j] * width, width), slim)],
            down_edge.at[:, pl.ds((subs - 1 - j) * slim, slim)],
            down_sem.at[subs],
        )
        for j in range(subs)
    ])
    for j in reversed(range(subs)):
        span = pl.ds(pl.multiple_of(quarters[j] * width + slim, slim), width - slim)
        loads.append([pltpu.make_async_copy(down_hbm.at[part, :, span], down_rest.at[j], down_sem.at[j])])

    def load(count):
        for group in loads[:count]:
            for copy in group:
                copy.start()
        del loads[:count]

    for copy in small:
        copy.wait()
    load(AHEAD)

    lines = E * CAP
    line = lax.broadcasted_iota(jnp.int32, (lines, block_rows), 0)
    expert, place = line // CAP, line % CAP
    first = jnp.broadcast_to(ids[0:1, :], (lines, block_rows)) == expert
    second = jnp.broadcast_to(ids[1:2, :], (lines, block_rows)) == expert
    named = jnp.where(first | second, 1.0, 0.0).astype(F32)
    before = lax.broadcasted_iota(jnp.int32, (block_rows, block_rows), 0) < lax.broadcasted_iota(
        jnp.int32, (block_rows, block_rows), 1
    )
    rank = jnp.dot(named.astype(BF16), jnp.where(before, 1.0, 0.0).astype(BF16), preferred_element_type=F32)
    here = jnp.where(rank == place.astype(F32), named, 0.0)
    chosen = here.astype(BF16)
    placed[...] = here

    half = width // 2
    spans_in = [(0, 0, near), (0, near, width - near)]
    for j in range(1, subs):
        spans_in += [(j, half, half), (j, near, half - near)]

    def pick(j, start, size):
        span = pl.ds(start, size)
        sent = jnp.dot(chosen, taken[j, :, span], preferred_element_type=F32)
        picked[j, :, :, span] = sent.astype(BF16).reshape(plane, CAP, size)

    def spread(n):
        j, start, size = spans_in[n]
        span = pl.ds(start, size)
        for k in reversed(range(1, plane)):
            send(
                picked.at[j, peers[k], :, span], rows.at[j, mine, :, span],
                pick_send.at[min(n, 1)], pick_recv.at[n], at(peers[k], sub),
            ).start()
        rows[j, mine, :, span] = picked[j, mine, :, span]

    pick(0, 0, width)
    with scope("barrier"):
        pl.semaphore_wait(barrier, plane + subs - 2)

    tok_copies = {}
    for j in range(1, subs):
        tok_copies[j] = send(
            taken.at[0, :, far], taken.at[j, :, far], tok_send, tok_recv.at[j - 1], at(mine, quarters[j])
        )
        tok_copies[j].start()
    spread(0)
    spread(1)

    def gathered(n):
        j, start, size = spans_in[n]
        arrived(rows.at[j, others, :, pl.ds(start, size)], pick_recv.at[n])

    with scope("pick0"):
        gathered(0)
    relays = {}
    for j in range(1, subs):
        relays[j] = send(
            rows.at[0, :, :, pl.ds(0, near)], rows.at[j, :, :, pl.ds(0, near)],
            relay_send, relay_recv.at[j - 1], at(mine, quarters[j]),
        )
        relays[j].start()
    spans_used = [(0, 0, width, 1)]
    for j in range(1, subs - 1):
        spans_used += [(j, half, half, 2 * j), (j, 0, half, 2 * j + 1)]
    last = 2 * (subs - 1)
    spans_used += [(subs - 1, half, half, last), (subs - 1, 0, near, None), (subs - 1, near, half - near, last + 1)]

    def absorb(n):
        j, start, size, source = spans_used[n]
        if start == half or j == 0:
            with scope(f"load{j}"):
                arrived(both.at[:, j], load_sem.at[j])
            load(2)
        if start == 0 and j > 0:
            with scope(f"relay{j}"):
                relays[j].wait_recv()
        if source is not None:
            with scope(f"pick{source}"):
                gathered(source)
        depth = pl.ds(start, size)

        def tile(span):
            x = rows[j, :, :, depth].reshape(plane * CAP, size)
            g = jnp.dot(x, both[0, j, depth, span], preferred_element_type=F32)
            u = jnp.dot(x, both[1, j, depth, span], preferred_element_type=F32)
            if n > 0:
                g = g + gate_sum[:, span]
                u = u + up_sum[:, span]
            if n < len(spans_used) - 1:
                gate_sum[:, span] = g
                up_sum[:, span] = u
            else:
                hidden[:, span] = (g / (1.0 + jnp.exp(-g)) * u).astype(BF16)

        with scope(f"absorb{n}"):
            for step in range(units // TILE):
                tile(pl.ds(step * TILE, TILE))

    for j in range(1, subs):
        if j == subs - 1:
            absorb(0)
        with scope(f"tok{j}"):
            tok_copies[j].wait_recv()
        pick(j, near, width - near)
        spread(2 * j)
        spread(2 * j + 1)
    for n in range(1, len(spans_used) - 1):
        absorb(n)
    load(len(loads))
    with scope("downwait"):
        arrived(down_edge, down_sem.at[subs])
        arrived(down_rest.at[subs - 1], down_sem.at[subs - 1])
    absorb(len(spans_used) - 1)

    edge_copies = {}
    mix_copies = {}

    def ship(n, j, span):
        for k in reversed(range(1, plane)):
            send(
                made.at[j, peers[k], :, span], home.at[j, mine, :, span],
                made_send.at[1 if n == subs else 0], made_recv.at[n], at(peers[k], sub),
            ).start()
        home[j, mine, :, span] = made[j, mine, :, span]

    def collect(n, j, span):
        with scope(f"made{n}"):
            arrived(home.at[j, others, :, span], made_recv.at[n])

    def combine(j, span):
        block = home[j, :, :, span].reshape(plane * CAP, span.size)
        return jnp.dot(weight_high, block, preferred_element_type=F32) + jnp.dot(
            weight_low, block, preferred_element_type=F32
        )

    def strip(first, count):
        begin = subs - 1 - first
        product = jnp.dot(
            hidden[...], down_edge[:, begin * slim : (begin + count) * slim], preferred_element_type=F32
        )
        for n, i in enumerate(range(first, first - count, -1)):
            part_sum = product[:, n * slim : (n + 1) * slim]
            if i == 0:
                edge_sum[...] = part_sum
                continue
            made[i, :, :, edge] = part_sum.astype(BF16).reshape(plane, CAP, slim)
            edge_copies[i] = send(
                made.at[i, :, :, edge], edges.at[i], edge_send, edge_recv.at[i - 1], at(mine, quarters[i])
            )
            edge_copies[i].start()

    def project(n, j, start, size):
        product = jnp.dot(hidden[...], down_rest[j, :, start - slim : start - slim + size], preferred_element_type=F32)
        made[j, :, :, pl.ds(start, size)] = product.astype(BF16).reshape(plane, CAP, size)
        ship(n, j, pl.ds(start, size))

    top = subs - 1
    with scope("strip0"):
        strip(top, subs // 2)
    with scope("proj0"):
        project(subs + 1, top, slim, half)
    with scope("strip1"):
        strip(top - subs // 2, subs - subs // 2)
    with scope("proj1"):
        project(top, top, slim + half, width - slim - half)
    for j in reversed(range(top)):
        with scope(f"down{j}"):
            arrived(down_rest.at[j], down_sem.at[j])
            project(j, j, slim, width - slim)

    first = jnp.broadcast_to(ids[0:1, :], (lines, block_rows)) == line // CAP
    level = levels[...].astype(F32) + 1.0
    share = level / (level[0:1, :] + level[1:2, :])
    weight = placed[...] * jnp.where(
        first,
        jnp.broadcast_to(share[0:1, :], (lines, block_rows)),
        jnp.broadcast_to(share[1:2, :], (lines, block_rows)),
    )
    weight = weight.T
    weight_high = weight.astype(BF16)
    weight_low = (weight - weight_high.astype(F32)).astype(BF16)

    def mix(j):
        if j == top:
            collect(subs + 1, j, pl.ds(slim, half))
            collect(j, j, pl.ds(slim + half, width - slim - half))
        else:
            collect(j, j, rest)
        mixed[j] = combine(j, rest).astype(BF16)
        mix_copies[j] = send(mixed.at[j], landed.at[j], mix_send, mix_recv.at[j - 1], at(mine, quarters[j]))
        mix_copies[j].start()

    for j in reversed(range(2, subs)):
        mix(j)
    sums = edge_sum[...]
    with scope("edgewait"):
        for j in range(1, subs):
            edge_copies[j].wait_recv()
            sums = sums + edges[j].reshape(plane * CAP, slim).astype(F32)
    made[0, :, :, edge] = sums.astype(BF16).reshape(plane, CAP, slim)
    ship(subs, 0, edge)
    mix(1)
    collect(0, 0, rest)
    total = combine(0, rest)
    for j in reversed(range(1, subs)):
        with scope(f"mixwait{j}"):
            mix_copies[j].wait_recv()
        total = total + landed[j].astype(F32)
    out[:, rest] = total.astype(BF16)
    collect(subs, 0, edge)
    out[:, edge] = combine(0, edge).astype(BF16)

    with scope("sends"):
        remote = pl.ds(1, subs - 1)
        departed(taken.at[remote, :, far], tok_send)
        departed(rows.at[remote, :, :, pl.ds(0, near)], relay_send)
        departed(edges.at[remote], edge_send)
        departed(landed.at[remote], mix_send)
        departed(rows.at[0, others, :, pl.ds(0, near)], pick_send.at[0])
        departed(rows.at[:, others, :, far], pick_send.at[1])
        departed(home.at[:, others, :, rest], made_send.at[0])
        departed(home.at[0, others, :, edge], made_send.at[1])


def shared_shards(parts, blks, subs, tokens, expert_ids, gate_level, gate_weight, up_weight, down_weight):
    block_rows, width = tokens.shape
    plane = parts * blks
    units = gate_weight.shape[2]
    vmem = pl.BlockSpec(memory_space=pltpu.VMEM)
    hbm = pl.BlockSpec(memory_space=pl.ANY)
    dma = pltpu.SemaphoreType.DMA
    return pl.pallas_call(
        functools.partial(fused, parts, blks, subs),
        out_shape=pltpu.VMEM((block_rows, width), BF16),
        in_specs=[hbm] * 6,
        out_specs=vmem,
        scratch_shapes=[
            pltpu.VMEM(expert_ids.T.shape, jnp.int32),
            pltpu.VMEM(gate_level.T.shape, jnp.int32),
            pltpu.VMEM((subs, block_rows, width), BF16),
            pltpu.VMEM((subs, plane, CAP, width), BF16),
            pltpu.VMEM((subs, plane, CAP, width), BF16),
            pltpu.VMEM((2, subs, width, units), BF16),
            pltpu.VMEM((subs, units, width - width * SLIM // 8), BF16),
            pltpu.VMEM((units, subs * (width * SLIM // 8)), BF16),
            pltpu.VMEM((plane * CAP, units), F32),
            pltpu.VMEM((plane * CAP, units), F32),
            pltpu.VMEM((plane * CAP, units), BF16),
            pltpu.VMEM((subs, plane, CAP, width), BF16),
            pltpu.VMEM((subs, plane, CAP, width), BF16),
            pltpu.VMEM((subs, block_rows, width - width * SLIM // 8), BF16),
            pltpu.VMEM((subs, block_rows, width - width * SLIM // 8), BF16),
            pltpu.VMEM((plane * CAP, width * SLIM // 8), F32),
            pltpu.VMEM((subs, plane, CAP, width * SLIM // 8), BF16),
            pltpu.VMEM((E * CAP, block_rows), F32),
            dma((subs,)), dma((subs + 1,)), dma((3,)),
            dma, dma((subs - 1,)),
            dma((2,)), dma((2 * subs,)),
            dma((2,)), dma((subs + 2,)),
            dma, dma((subs - 1,)),
            dma, dma((subs - 1,)),
            dma, dma((subs - 1,)),
        ],
        compiler_params=pltpu.CompilerParams(
            collective_id=0, has_side_effects=True, vmem_limit_bytes=65000000
        ),
    )(tokens, expert_ids.T, gate_level.T, gate_weight, up_weight, down_weight)


def routed(parts, blks, subs, tokens, expert_ids, gate_level, gate_weight, up_weight, down_weight):
    plane = parts * blks
    width = tokens.shape[1]
    units = gate_weight.shape[2]
    fits = gate_weight.shape[0] == parts and plane == E and plane & (plane - 1) == 0
    fits = fits and subs > 1 and subs & (subs - 1) == 0 and width % TILE == 0 and units % TILE == 0
    fits = fits and tokens.shape[0] == 2 * CAP
    arrays = (tokens, expert_ids, gate_level, gate_weight, up_weight, down_weight)
    return shared_shards(parts, blks, subs, *arrays) if fits else shards(*arrays)


def solution(mesh):
    sizes = (mesh.shape["parts"], mesh.shape["blk"], mesh.shape["sub"])
    return jax.shard_map(
        functools.partial(routed, *sizes),
        mesh=mesh,
        in_specs=(
            P(("parts", "blk"), "sub"),
            P(("parts", "blk"), None),
            P(("parts", "blk"), None),
            P("blk", None, "sub"),
            P("blk", None, "sub"),
            P("blk", "sub", None),
        ),
        out_specs=P(("parts", "blk"), "sub"),
        check_vma=False,
    )
```

```python
import contextlib
import functools

import jax
import jax.numpy as jnp
from jax import lax
from jax.sharding import PartitionSpec as P

from jax.experimental import pallas as pl
from jax.experimental.pallas import tpu as pltpu

E = 8
TOP = 2
CAP = 16
BF16 = jnp.bfloat16
F32 = jnp.float32
TILE = 1024
AHEAD = 3
NEAR = 2
SLIM = 2
SCOPES = False


def scope(name):
    return jax.named_scope(name) if SCOPES else contextlib.nullcontext()


def shards(tokens, expert_ids, gate_level, gate_weight, up_weight, down_weight):
    block_count = lax.axis_size("blk")
    sub_count = lax.axis_size("sub")
    local_slots = gate_weight.shape[0]
    hidden_width = gate_weight.shape[2]
    slot_count = local_slots * block_count
    halves = slot_count // E
    token_rows = tokens.shape[0]
    feature_width = tokens.shape[1]
    buffer_width = slot_count * CAP
    received_rows = block_count * CAP
    picked = expert_ids.reshape(-1)
    onehot = (picked[:, None] == jnp.arange(E, dtype=jnp.int32)[None, :]).astype(jnp.int32)
    ranking = jnp.sum((jnp.cumsum(onehot, axis=0) - onehot) * onehot, axis=1)
    columns = (
        picked[:, None] * CAP
        + (jnp.arange(halves, dtype=jnp.int32) * E)[None, :] * CAP
        + ranking[:, None]
    )
    columns = columns.reshape(token_rows, TOP * halves)
    matches = columns[:, :, None] == jnp.arange(buffer_width, dtype=jnp.int32)[None, None, :]
    levels = gate_level.astype(jnp.float32) + 1.0
    shares = levels / jnp.sum(levels, axis=1, keepdims=True)
    shares_wide = jnp.repeat(shares, halves, axis=1)
    combine_weights = jnp.sum(matches.astype(jnp.float32) * shares_wide[:, :, None], axis=1)
    chosen = jnp.any(matches, axis=1).astype(jnp.bfloat16)
    outgoing = lax.dot_general(
        chosen, tokens, (((0,), (0,)), ((), ())), preferred_element_type=jnp.float32
    )
    outgoing = outgoing.astype(jnp.bfloat16).reshape(slot_count, CAP, feature_width)
    copies = jnp.broadcast_to(
        outgoing.reshape(block_count, 1, local_slots, CAP, feature_width),
        (block_count, sub_count, local_slots, CAP, feature_width),
    )
    copies = copies.reshape(block_count * sub_count, local_slots, CAP, feature_width)
    arrived = lax.all_to_all(copies, ("blk", "sub"), split_axis=0, concat_axis=0, tiled=True)
    arrived = arrived.reshape(block_count, sub_count, local_slots, CAP, feature_width)
    gate_split = gate_weight.reshape(local_slots, sub_count, feature_width, hidden_width)
    up_split = up_weight.reshape(local_slots, sub_count, feature_width, hidden_width)
    gate_acts = jnp.einsum(
        "bsncd,nsdf->nbcf", arrived, gate_split, preferred_element_type=jnp.float32
    )
    up_acts = jnp.einsum("bsncd,nsdf->nbcf", arrived, up_split, preferred_element_type=jnp.float32)
    gate_acts = gate_acts.reshape(local_slots, received_rows, hidden_width)
    up_acts = up_acts.reshape(local_slots, received_rows, hidden_width)
    hidden = (jax.nn.silu(gate_acts) * up_acts).astype(jnp.bfloat16)
    full_out = jnp.einsum("nrf,nfd->nrd", hidden, down_weight, preferred_element_type=jnp.float32)
    local_out = lax.psum_scatter(
        full_out.astype(jnp.bfloat16), "sub", scatter_dimension=2, tiled=True
    )
    home_rows = lax.all_to_all(local_out, "blk", split_axis=1, concat_axis=0, tiled=True)
    home_flat = home_rows.reshape(buffer_width, feature_width).astype(jnp.float32)
    mixed_out = jnp.dot(
        combine_weights,
        home_flat,
        precision=lax.Precision.HIGHEST,
        preferred_element_type=jnp.float32,
    )
    return mixed_out.astype(jnp.bfloat16)


def flip(index, mask, count):
    total, bit = 0, 1
    while bit < count:
        digit = (index // bit) % 2
        total = total + bit * ((1 - digit) if mask & bit else digit)
        bit *= 2
    return total


def fused(
    parts, blks, subs, tokens_hbm, ids_hbm, levels_hbm, gate_hbm, up_hbm, down_hbm, out,
    ids, levels, taken, picked, rows, both, down_rest, down_edge, gate_sum, up_sum, hidden, made, home, mixed, landed, edge_sum, edges, placed,
    load_sem, down_sem, own_sem, tok_send, tok_recv, pick_send, pick_recv, made_send, made_recv, mix_send, mix_recv, relay_send, relay_recv, edge_send, edge_recv,
):
    plane = parts * blks
    part, blk, sub = lax.axis_index("parts"), lax.axis_index("blk"), lax.axis_index("sub")
    mine = blk * parts + part
    block_rows, width = tokens_hbm.shape
    units = hidden.shape[1]

    def at(slot, depth):
        return {"parts": slot % parts, "blk": slot // parts, "sub": depth}

    near = width * NEAR // 8
    far = pl.ds(near, width - near)
    quarters = [flip(sub, j, subs) for j in range(subs)]
    peers = [flip(mine, k, plane) for k in range(plane)]

    def send(source, target, send_sem, recv_sem, to):
        return pltpu.make_async_remote_copy(
            src_ref=source, dst_ref=target, send_sem=send_sem, recv_sem=recv_sem,
            device_id=to, device_id_type=pl.DeviceIdType.MESH,
        )

    def arrived(ref, sem):
        send(ref, ref, sem, sem, at(mine, sub)).wait_recv()

    def departed(ref, sem):
        send(ref, ref, sem, sem, at(mine, sub)).wait_send()

    others = pl.ds(0, plane - 1)
    barrier = pltpu.get_barrier_semaphore()
    for k in range(1, plane):
        pl.semaphore_signal(barrier, inc=1, device_id=at(peers[k], sub), device_id_type=pl.DeviceIdType.MESH)
    for j in range(1, subs):
        pl.semaphore_signal(barrier, inc=1, device_id=at(mine, quarters[j]), device_id_type=pl.DeviceIdType.MESH)
    small = [
        pltpu.make_async_copy(source, target, own_sem.at[n])
        for n, (source, target) in enumerate([(ids_hbm, ids), (levels_hbm, levels), (tokens_hbm, taken.at[0])])
    ]
    for copy in small:
        copy.start()

    slim = width * SLIM // 8
    edge, rest = pl.ds(0, slim), pl.ds(slim, width - slim)
    loads = []
    for j in range(subs):
        span = pl.ds(pl.multiple_of(quarters[j] * width, width), width)
        loads.append([
            pltpu.make_async_copy(source.at[part, span, :], both.at[i, j], load_sem.at[j])
            for i, source in enumerate((gate_hbm, up_hbm))
        ])
    loads.append([
        pltpu.make_async_copy(
            down_hbm.at[part, :, pl.ds(pl.multiple_of(quarters[j] * width, width), slim)],
            down_edge.at[:, pl.ds((subs - 1 - j) * slim, slim)],
            down_sem.at[subs],
        )
        for j in range(subs)
    ])
    for j in reversed(range(subs)):
        span = pl.ds(pl.multiple_of(quarters[j] * width + slim, slim), width - slim)
        loads.append([pltpu.make_async_copy(down_hbm.at[part, :, span], down_rest.at[j], down_sem.at[j])])

    def load(count):
        for group in loads[:count]:
            for copy in group:
                copy.start()
        del loads[:count]

    for copy in small:
        copy.wait()

    lines = E * CAP
    line = lax.broadcasted_iota(jnp.int32, (lines, block_rows), 0)
    expert, place = line // CAP, line % CAP
    first = jnp.broadcast_to(ids[0:1, :], (lines, block_rows)) == expert
    second = jnp.broadcast_to(ids[1:2, :], (lines, block_rows)) == expert
    named = jnp.where(first | second, 1.0, 0.0).astype(F32)
    before = lax.broadcasted_iota(jnp.int32, (block_rows, block_rows), 0) < lax.broadcasted_iota(
        jnp.int32, (block_rows, block_rows), 1
    )
    rank = jnp.dot(named.astype(BF16), jnp.where(before, 1.0, 0.0).astype(BF16), preferred_element_type=F32)
    here = jnp.where(rank == place.astype(F32), named, 0.0)
    chosen = here.astype(BF16)
    placed[...] = here

    half = width // 2
    spans_in = [(0, 0, near), (0, near, width - near)]
    for j in range(1, subs):
        spans_in += [(j, half, half), (j, near, half - near)]

    def pick(j, start, size):
        span = pl.ds(start, size)
        sent = jnp.dot(chosen, taken[j, :, span], preferred_element_type=F32)
        picked[j, :, :, span] = sent.astype(BF16).reshape(plane, CAP, size)

    def spread(n):
        j, start, size = spans_in[n]
        span = pl.ds(start, size)
        for k in reversed(range(1, plane)):
            send(
                picked.at[j, peers[k], :, span], rows.at[j, mine, :, span],
                pick_send.at[min(n, 1)], pick_recv.at[n], at(peers[k], sub),
            ).start()
        rows[j, mine, :, span] = picked[j, mine, :, span]

    pick(0, 0, near)
    load(AHEAD)
    with scope("barrier"):
        pl.semaphore_wait(barrier, plane + subs - 2)

    tok_copies = {}
    for j in range(1, subs):
        tok_copies[j] = send(
            taken.at[0, :, far], taken.at[j, :, far], tok_send, tok_recv.at[j - 1], at(mine, quarters[j])
        )
        tok_copies[j].start()
    spread(0)
    pick(0, near, width - near)
    spread(1)

    def gathered(n):
        j, start, size = spans_in[n]
        arrived(rows.at[j, others, :, pl.ds(start, size)], pick_recv.at[n])

    with scope("pick0"):
        gathered(0)
    relays = {}
    for j in range(1, subs):
        relays[j] = send(
            rows.at[0, :, :, pl.ds(0, near)], rows.at[j, :, :, pl.ds(0, near)],
            relay_send, relay_recv.at[j - 1], at(mine, quarters[j]),
        )
        relays[j].start()
    spans_used = [(0, 0, width, 1)]
    for j in range(1, subs - 1):
        spans_used += [(j, half, half, 2 * j), (j, 0, half, 2 * j + 1)]
    last = 2 * (subs - 1)
    spans_used += [(subs - 1, half, half, last), (subs - 1, 0, near, None), (subs - 1, near, half - near, last + 1)]

    def absorb(n):
        j, start, size, source = spans_used[n]
        if start == half or j == 0:
            with scope(f"load{j}"):
                arrived(both.at[:, j], load_sem.at[j])
            load(2)
        if start == 0 and j > 0:
            with scope(f"relay{j}"):
                relays[j].wait_recv()
        if source is not None:
            with scope(f"pick{source}"):
                gathered(source)
        depth = pl.ds(start, size)

        def tile(span):
            x = rows[j, :, :, depth].reshape(plane * CAP, size)
            g = jnp.dot(x, both[0, j, depth, span], preferred_element_type=F32)
            u = jnp.dot(x, both[1, j, depth, span], preferred_element_type=F32)
            if n > 0:
                g = g + gate_sum[:, span]
                u = u + up_sum[:, span]
            if n < len(spans_used) - 1:
                gate_sum[:, span] = g
                up_sum[:, span] = u
            else:
                hidden[:, span] = (g / (1.0 + jnp.exp(-g)) * u).astype(BF16)

        with scope(f"absorb{n}"):
            for step in range(units // TILE):
                tile(pl.ds(step * TILE, TILE))

    for j in range(1, subs):
        if j == subs - 1:
            absorb(0)
        with scope(f"tok{j}"):
            tok_copies[j].wait_recv()
        pick(j, near, width - near)
        spread(2 * j)
        spread(2 * j + 1)
    for n in range(1, len(spans_used) - 1):
        absorb(n)
    load(len(loads))
    with scope("downwait"):
        arrived(down_edge, down_sem.at[subs])
        arrived(down_rest.at[subs - 1], down_sem.at[subs - 1])
    absorb(len(spans_used) - 1)

    edge_copies = {}
    mix_copies = {}

    def ship(n, j, span):
        for k in reversed(range(1, plane)):
            send(
                made.at[j, peers[k], :, span], home.at[j, mine, :, span],
                made_send.at[1 if n == subs else 0], made_recv.at[n], at(peers[k], sub),
            ).start()
        home[j, mine, :, span] = made[j, mine, :, span]

    def collect(n, j, span):
        with scope(f"made{n}"):
            arrived(home.at[j, others, :, span], made_recv.at[n])

    def combine(j, span):
        block = home[j, :, :, span].reshape(plane * CAP, span.size)
        return jnp.dot(weight_high, block, preferred_element_type=F32) + jnp.dot(
            weight_low, block, preferred_element_type=F32
        )

    def strip(first, count):
        begin = subs - 1 - first
        product = jnp.dot(
            hidden[...], down_edge[:, begin * slim : (begin + count) * slim], preferred_element_type=F32
        )
        for n, i in enumerate(range(first, first - count, -1)):
            part_sum = product[:, n * slim : (n + 1) * slim]
            if i == 0:
                edge_sum[...] = part_sum
                continue
            made[i, :, :, edge] = part_sum.astype(BF16).reshape(plane, CAP, slim)
            edge_copies[i] = send(
                made.at[i, :, :, edge], edges.at[i], edge_send, edge_recv.at[i - 1], at(mine, quarters[i])
            )
            edge_copies[i].start()

    def project(n, j, start, size):
        product = jnp.dot(hidden[...], down_rest[j, :, start - slim : start - slim + size], preferred_element_type=F32)
        made[j, :, :, pl.ds(start, size)] = product.astype(BF16).reshape(plane, CAP, size)
        ship(n, j, pl.ds(start, size))

    top = subs - 1
    with scope("strip0"):
        strip(top, subs // 2)
    with scope("proj0"):
        project(subs + 1, top, slim, half)
    with scope("strip1"):
        strip(top - subs // 2, subs - subs // 2)
    with scope("proj1"):
        project(top, top, slim + half, width - slim - half)
    for j in reversed(range(top)):
        with scope(f"down{j}"):
            arrived(down_rest.at[j], down_sem.at[j])
            if j == 1:
                project(subs + 2, j, slim, half)
                project(j, j, slim + half, width - slim - half)
            else:
                project(j, j, slim, width - slim)

    first = jnp.broadcast_to(ids[0:1, :], (lines, block_rows)) == line // CAP
    level = levels[...].astype(F32) + 1.0
    share = level / (level[0:1, :] + level[1:2, :])
    weight = placed[...] * jnp.where(
        first,
        jnp.broadcast_to(share[0:1, :], (lines, block_rows)),
        jnp.broadcast_to(share[1:2, :], (lines, block_rows)),
    )
    weight = weight.T
    weight_high = weight.astype(BF16)
    weight_low = (weight - weight_high.astype(F32)).astype(BF16)

    def post(j, m, start, size):
        span = pl.ds(start - slim, size)
        mixed[j, :, span] = combine(j, pl.ds(start, size)).astype(BF16)
        copy = send(mixed.at[j, :, span], landed.at[j, :, span], mix_send, mix_recv.at[m], at(mine, quarters[j]))
        copy.start()
        mix_copies.setdefault(j, []).append(copy)

    def mix(j):
        if j == 1:
            collect(subs + 2, j, pl.ds(slim, half))
            post(j, 0, slim, half)
            collect(j, j, pl.ds(slim + half, width - slim - half))
            post(j, subs - 1, slim + half, width - slim - half)
            return
        if j == top:
            collect(subs + 1, j, pl.ds(slim, half))
            collect(j, j, pl.ds(slim + half, width - slim - half))
        else:
            collect(j, j, rest)
        post(j, j - 1, slim, width - slim)

    for j in reversed(range(2, subs)):
        mix(j)
    sums = edge_sum[...]
    with scope("edgewait"):
        for j in range(1, subs):
            edge_copies[j].wait_recv()
            sums = sums + edges[j].reshape(plane * CAP, slim).astype(F32)
    made[0, :, :, edge] = sums.astype(BF16).reshape(plane, CAP, slim)
    ship(subs, 0, edge)
    mix(1)
    collect(0, 0, rest)
    total = combine(0, rest)
    for j in reversed(range(1, subs)):
        with scope(f"mixwait{j}"):
            for copy in mix_copies[j]:
                copy.wait_recv()
        total = total + landed[j].astype(F32)
    out[:, rest] = total.astype(BF16)
    collect(subs, 0, edge)
    out[:, edge] = combine(0, edge).astype(BF16)

    with scope("sends"):
        remote = pl.ds(1, subs - 1)
        departed(taken.at[remote, :, far], tok_send)
        departed(rows.at[remote, :, :, pl.ds(0, near)], relay_send)
        departed(edges.at[remote], edge_send)
        departed(landed.at[remote], mix_send)
        departed(rows.at[0, others, :, pl.ds(0, near)], pick_send.at[0])
        departed(rows.at[:, others, :, far], pick_send.at[1])
        departed(home.at[:, others, :, rest], made_send.at[0])
        departed(home.at[0, others, :, edge], made_send.at[1])


def shared_shards(parts, blks, subs, tokens, expert_ids, gate_level, gate_weight, up_weight, down_weight):
    block_rows, width = tokens.shape
    plane = parts * blks
    units = gate_weight.shape[2]
    vmem = pl.BlockSpec(memory_space=pltpu.VMEM)
    hbm = pl.BlockSpec(memory_space=pl.ANY)
    dma = pltpu.SemaphoreType.DMA
    return pl.pallas_call(
        functools.partial(fused, parts, blks, subs),
        out_shape=pltpu.VMEM((block_rows, width), BF16),
        in_specs=[hbm] * 6,
        out_specs=vmem,
        scratch_shapes=[
            pltpu.VMEM(expert_ids.T.shape, jnp.int32),
            pltpu.VMEM(gate_level.T.shape, jnp.int32),
            pltpu.VMEM((subs, block_rows, width), BF16),
            pltpu.VMEM((subs, plane, CAP, width), BF16),
            pltpu.VMEM((subs, plane, CAP, width), BF16),
            pltpu.VMEM((2, subs, width, units), BF16),
            pltpu.VMEM((subs, units, width - width * SLIM // 8), BF16),
            pltpu.VMEM((units, subs * (width * SLIM // 8)), BF16),
            pltpu.VMEM((plane * CAP, units), F32),
            pltpu.VMEM((plane * CAP, units), F32),
            pltpu.VMEM((plane * CAP, units), BF16),
            pltpu.VMEM((subs, plane, CAP, width), BF16),
            pltpu.VMEM((subs, plane, CAP, width), BF16),
            pltpu.VMEM((subs, block_rows, width - width * SLIM // 8), BF16),
            pltpu.VMEM((subs, block_rows, width - width * SLIM // 8), BF16),
            pltpu.VMEM((plane * CAP, width * SLIM // 8), F32),
            pltpu.VMEM((subs, plane, CAP, width * SLIM // 8), BF16),
            pltpu.VMEM((E * CAP, block_rows), F32),
            dma((subs,)), dma((subs + 1,)), dma((3,)),
            dma, dma((subs - 1,)),
            dma((2,)), dma((2 * subs,)),
            dma((2,)), dma((subs + 3,)),
            dma, dma((subs,)),
            dma, dma((subs - 1,)),
            dma, dma((subs - 1,)),
        ],
        compiler_params=pltpu.CompilerParams(
            collective_id=0, has_side_effects=True, vmem_limit_bytes=65000000
        ),
    )(tokens, expert_ids.T, gate_level.T, gate_weight, up_weight, down_weight)


def routed(parts, blks, subs, tokens, expert_ids, gate_level, gate_weight, up_weight, down_weight):
    plane = parts * blks
    width = tokens.shape[1]
    units = gate_weight.shape[2]
    fits = gate_weight.shape[0] == parts and plane == E and plane & (plane - 1) == 0
    fits = fits and subs > 2 and subs & (subs - 1) == 0 and width % TILE == 0 and units % TILE == 0
    fits = fits and tokens.shape[0] == 2 * CAP
    arrays = (tokens, expert_ids, gate_level, gate_weight, up_weight, down_weight)
    return shared_shards(parts, blks, subs, *arrays) if fits else shards(*arrays)


def solution(mesh):
    sizes = (mesh.shape["parts"], mesh.shape["blk"], mesh.shape["sub"])
    return jax.shard_map(
        functools.partial(routed, *sizes),
        mesh=mesh,
        in_specs=(
            P(("parts", "blk"), "sub"),
            P(("parts", "blk"), None),
            P(("parts", "blk"), None),
            P("blk", None, "sub"),
            P("blk", None, "sub"),
            P("blk", "sub", None),
        ),
        out_specs=P(("parts", "blk"), "sub"),
        check_vma=False,
    )
```
